32 devices in a mesh: ep: 8 (over z, x), tp: 4 (over y, core).
Axes of the slice: x: 2, y: 2, z: 4, core: 2. Of those that a mesh axis runs over, the one named last changes fastest.
Arguments:
- hidden: bfloat16 [512, 2880], P('ep'), may hold values from -0.59765625 to 0.59765625
- queries: bfloat16 [512, 2048], P('ep', 'tp'), may hold values from -160 to 160
- new_keys: bfloat16 [512, 256], P('ep', 'tp'), may hold values from -6 to 6
- new_values: bfloat16 [512, 256], P('ep', 'tp'), may hold values from -6 to 6
- key_cache: bfloat16 [64, 4, 64, 1024], P('ep', 'tp'), may hold values from -6 to 6
- value_cache: bfloat16 [64, 4, 64, 1024], P('ep', 'tp'), may hold values from -6 to 6
- cache_lengths: int32 [64], P('ep'), may hold values from 16 to 1024
- w_out: bfloat16 [2048, 2880], P('tp'), may hold values from -0.125 to 0.125
- w_router: bfloat16 [2880, 8], replicated, may hold values from -0.109375 to 0.109375
- routes: int32 [512, 4], P('ep'), may hold values from 0 to 7, all different within a row; in each aligned block of 16 rows (0 to 15, 16 to 31, ...) at most 16 rows name the same one
- w_gate: bfloat16 [8, 2880, 1536], P('ep', None, 'tp'), may hold values from -0.109375 to 0.109375
- w_up: bfloat16 [8, 2880, 1536], P('ep', None, 'tp'), may hold values from -0.109375 to 0.109375
- w_down: bfloat16 [8, 1536, 2880], P('ep', 'tp'), may hold values from -0.15625 to 0.15625
Outputs:
- layer_out: bfloat16 [512, 2880], P(('ep', 'tp'))
The draws below stay inside these ranges and needn't reach their ends.
Inputs may be any that keep to these rules, and one draw needn't show every extreme that they name: `routes`: each token names 4 different experts; in each aligned block of 16 tokens no expert is named by more than 16 tokens, and in some blocks one expert is named by exactly 16.
All inputs are finite; a program needn't handle non-finite values.
Results may differ from the reference program's by a relative error of at most 0.02.
Values may be sent and summed in bfloat16 or wider, within the bound.
A program may use at most 64 MiB of HBM per device.

```python
import math
import jax
import jax.numpy as jnp
import numpy as np
from jax import lax

D = 2880
HEADS = 32
KV_HEADS = 4
HEAD_DIM = 64
FF = 1536
TOP = 4
SEQ_DEV = 8
LEN = 1024
EXPERTS = 8
SEQS = 64
TOKENS = 512
TOK_EP = 64
BLOCK = 16
CAP = 16
N_EP = 8
N_TP = 4


def draw_queries(key, part):
    shape_q = (TOKENS, HEADS * HEAD_DIM)
    values = jnp.clip(jax.random.normal(jax.random.fold_in(key, 1), shape_q, jnp.float32), -6.0, 6.0)
    return values.astype(jnp.bfloat16)


def draw_key_cache(key, part):
    base_draw = jax.random.normal(jax.random.fold_in(key, 3), (SEQS, KV_HEADS, HEAD_DIM, LEN), jnp.float32)
    base_draw = jnp.clip(base_draw, -6.0, 6.0)
    return base_draw.astype(jnp.bfloat16)


def place_ends(array, stream_key, low, high):
    dims = array.shape
    index_at = [jax.random.randint(jax.random.fold_in(stream_key, axis), (), 0, dims[axis]) for axis in range(len(dims))]
    array = array.at[tuple(index_at)].set(low)
    longest = dims.index(max(dims))
    index_at[longest] = (index_at[longest] + 1) % dims[longest]
    return array.at[tuple(index_at)].set(high)


def levels(key, dims, cuts, low, largest):
    gain = 1.0
    for axis_at, parts in cuts:
        steps = jax.random.uniform(jax.random.fold_in(jax.random.fold_in(key, 6), axis_at), (parts,), jnp.float32, low / len(cuts), largest / len(cuts))
        gain = gain * jnp.repeat(jnp.exp(steps), dims[axis_at] // parts).reshape((-1,) + (1,) * (len(dims) - 1 - axis_at))
    return gain


def deal_out(stream_key, own, number, rows, amount, top, reach, lean):
    ranking = jax.random.permutation(stream_key, amount)
    packed, common = portions_of(amount, rows * top, reach, lean, True), portions_of(amount, rows * top, reach, lean, False)
    places = jnp.arange(amount)

    def named(lengths, turn):
        used = int((lengths > 0).sum())
        fixed = max(1, used // 4)
        passed = fixed + (places - fixed + turn * (used - fixed)) % max(1, amount - fixed)
        return jnp.zeros((amount,), jnp.int32).at[ranking[jnp.where(places < fixed, places, passed)]].set(jnp.asarray(lengths, jnp.int32))

    lengths = jnp.where(number % 4 == 0, named(packed, number // 4), named(common, number - number // 4 - 1))
    mixed = jax.random.permutation(jax.random.fold_in(own, 3), amount)
    giver, receiver = mixed[0:amount // 2 * 2:2], mixed[1:amount // 2 * 2:2]
    slack = jnp.minimum(lengths[giver] - 1, reach - lengths[receiver]) // 2
    slack = jnp.where((giver == ranking[0]) | (receiver == ranking[0]) | (lengths[receiver] == 0), 0, jnp.maximum(slack, 0))
    passed = jax.random.randint(jax.random.fold_in(own, 4), (amount // 2,), 0, 1 << 20) % (slack + 1)
    lengths = lengths.at[giver].add(-passed).at[receiver].add(passed)
    items = jnp.searchsorted(jnp.cumsum(lengths), jnp.arange(rows * top), side="right").astype(jnp.int32)
    table = items.reshape(top, rows).T
    table = table[jax.random.permutation(jax.random.fold_in(own, 1), rows)]
    turn = jax.random.randint(jax.random.fold_in(own, 2), (rows, 1), 0, top)
    return jnp.take_along_axis(table, (jnp.arange(top)[None, :] + turn) % top, axis=1)


def portions_of(count, total, most, slope, full):
    weights = [(1 << 20) // math.isqrt(standing ** slope) + 1 for standing in range(1, count + 1)]
    largest = most if full else min(most, max(-(-total // count), total * weights[0] // sum(weights)))
    least = 1 if total - largest >= count - 1 else 0
    holding, rest = [largest] + [least] * (count - 1), total - largest - least * (count - 1)
    while rest > 0:
        movable = [i for i in range(1, count) if holding[i] < largest] or [i for i in range(1, count) if holding[i] < most]
        mass, left = sum([weights[i] for i in movable]), rest
        for i in movable:
            extra = min(most - holding[i], max(1, left * weights[i] // mass), rest)
            holding[i] = holding[i] + extra
            rest = rest - extra
    return np.array(holding)


def centred(key, dims, width, limit, split=(), kind=jnp.bfloat16):
    values = jax.random.normal(key, dims, jnp.float32) * width
    if len(split) > 0:
        values = levels(key, dims, split, -0.22, 0.18) * values
    return jnp.clip(values, min=-limit, max=limit).astype(kind)


def setup_inputs(seed: int = 0) -> dict:
    keys = jax.random.split(jax.random.key(seed), 14)
    hidden = centred(keys[0], (TOKENS, D), 0.1, 0.59765625, ((0, 8),))
    queries = draw_queries(jax.random.fold_in(keys[13], 71), 0)
    new_keys = centred(keys[2], (TOKENS, KV_HEADS * HEAD_DIM), 1.0, 6.0, ((0, 8), (1, 4)))
    new_values = centred(keys[3], (TOKENS, KV_HEADS * HEAD_DIM), 1.0, 6.0, ((0, 8), (1, 4)))
    key_cache = draw_key_cache(jax.random.fold_in(keys[13], 71), 0)
    value_cache = centred(keys[5], (SEQS, KV_HEADS, HEAD_DIM, LEN), 1.0, 6.0, ((0, 8), (1, 4)))
    cache_lengths = place_ends(jax.random.randint(keys[6], (SEQS,), 16, LEN + 1), jax.random.fold_in(keys[6], 1), 16, LEN).astype(jnp.int32)
    w_out = centred(keys[7], (HEADS * HEAD_DIM, D), (HEADS * HEAD_DIM) ** -0.5, 0.125, ((0, 4),))
    w_router = centred(keys[8], (D, EXPERTS), D ** -0.5, 0.109375)
    routes_keys = jax.random.split(jax.random.fold_in(keys[9], 1), TOKENS // BLOCK)
    routes_turns = jax.random.permutation(jax.random.fold_in(keys[9], 3), TOKENS // BLOCK)
    routes = jax.vmap(lambda own, number: deal_out(jax.random.fold_in(keys[9], 2), own, number, BLOCK, EXPERTS, TOP, CAP, 2))(routes_keys, routes_turns).reshape((TOKENS, TOP))
    w_gate = centred(keys[10], (EXPERTS, D, FF), D ** -0.5, 0.109375, ((0, 8), (2, 4)))
    w_up = centred(keys[11], (EXPERTS, D, FF), D ** -0.5, 0.109375, ((0, 8), (2, 4)))
    w_down = centred(keys[12], (EXPERTS, FF, D), FF ** -0.5, 0.15625, ((0, 8), (1, 4)))
    return dict(hidden=hidden, queries=queries, new_keys=new_keys, new_values=new_values, key_cache=key_cache, value_cache=value_cache, cache_lengths=cache_lengths, w_out=w_out, w_router=w_router, routes=routes, w_gate=w_gate, w_up=w_up, w_down=w_down)


def attend_block(queries, new_keys, new_values, key_cache, value_cache, cache_lengths):
    seq_count, kv_count, head_dim, length = key_cache.shape
    new_count = queries.shape[0] // seq_count
    group_size = queries.shape[1] // (kv_count * head_dim)
    row_count = new_count * group_size
    scale = head_dim ** (-0.5)
    query_block = queries.astype(jnp.float32).reshape(seq_count, new_count, kv_count, group_size, head_dim)
    query_block = query_block.transpose(0, 2, 1, 3, 4).reshape(seq_count, kv_count, row_count, head_dim)
    fresh_keys = new_keys.astype(jnp.float32).reshape(seq_count, new_count, kv_count, head_dim).transpose(0, 2, 1, 3)
    fresh_values = new_values.astype(jnp.float32).reshape(seq_count, new_count, kv_count, head_dim).transpose(0, 2, 1, 3)
    cache_scores = jnp.einsum('skrd,skdl->skrl', query_block, key_cache.astype(jnp.float32)) * scale
    in_cache = jnp.arange(length)[None, :] < cache_lengths[:, None]
    cache_scores = jnp.where(in_cache[:, None, None, :], cache_scores, -1e+30)
    fresh_scores = jnp.einsum('skrd,sknd->skrn', query_block, fresh_keys) * scale
    causal = (jnp.arange(row_count) // group_size)[:, None] >= jnp.arange(new_count)[None, :]
    fresh_scores = jnp.where(causal[None, None, :, :], fresh_scores, -1e+30)
    row_max = jnp.maximum(lax.optimization_barrier(jnp.max(cache_scores, -1, keepdims=True)), lax.optimization_barrier(jnp.max(fresh_scores, -1, keepdims=True)))
    cache_exp = jnp.exp(cache_scores - row_max)
    fresh_exp = jnp.exp(fresh_scores - row_max)
    denom_sum = lax.optimization_barrier(jnp.sum(cache_exp, -1, keepdims=True)) + lax.optimization_barrier(jnp.sum(fresh_exp, -1, keepdims=True))
    cache_probs = (cache_exp / denom_sum).astype(jnp.bfloat16).astype(jnp.float32)
    fresh_probs = (fresh_exp / denom_sum).astype(jnp.bfloat16).astype(jnp.float32)
    head_mix = jnp.einsum('skrl,skdl->skrd', cache_probs, value_cache.astype(jnp.float32))
    head_mix = head_mix + jnp.einsum('skrn,sknd->skrd', fresh_probs, fresh_values)
    head_mix = head_mix.reshape(seq_count, kv_count, new_count, group_size, head_dim).transpose(0, 2, 1, 3, 4)
    return head_mix.reshape(seq_count * new_count, kv_count * group_size * head_dim).astype(jnp.bfloat16)

def expert_rows(pieces):
    buffer_rows, gate_weight, up_weight, down_weight = pieces
    gate_proj = jnp.dot(buffer_rows, gate_weight, preferred_element_type=jnp.float32)
    up_proj = jnp.dot(buffer_rows, up_weight, preferred_element_type=jnp.float32)
    activated = ((up_proj + 1.0) * gate_proj * jax.nn.sigmoid(1.702 * gate_proj)).astype(jnp.bfloat16)
    return jnp.dot(activated, down_weight, preferred_element_type=jnp.float32)

def reference(hidden, queries, new_keys, new_values, key_cache, value_cache, cache_lengths, w_out, w_router, routes, w_gate, w_up, w_down):
    blocks = (queries.reshape(N_EP, TOK_EP, HEADS * HEAD_DIM), new_keys.reshape(N_EP, TOK_EP, KV_HEADS * HEAD_DIM), new_values.reshape(N_EP, TOK_EP, KV_HEADS * HEAD_DIM), key_cache.reshape(N_EP, SEQ_DEV, KV_HEADS, HEAD_DIM, LEN), value_cache.reshape(N_EP, SEQ_DEV, KV_HEADS, HEAD_DIM, LEN), cache_lengths.reshape(N_EP, SEQ_DEV))
    attended = lax.map(lambda pieces: attend_block(*pieces), blocks).reshape(TOKENS, HEADS * HEAD_DIM)
    residual = hidden.astype(jnp.float32) + jnp.dot(attended, w_out, preferred_element_type=jnp.float32)
    normed = (residual * lax.rsqrt(lax.optimization_barrier(jnp.mean(residual * residual, -1, keepdims=True)) + 1e-05)).astype(jnp.bfloat16)
    logits = jnp.dot(normed, w_router, preferred_element_type=jnp.float32)
    picked = jnp.take_along_axis(logits, routes, 1)
    picked_exp = jnp.exp(picked)
    weights = picked_exp / lax.optimization_barrier(jnp.sum(picked_exp, -1, keepdims=True))
    flat_routes = routes.reshape(-1).astype(jnp.int32)
    one_hot = (flat_routes[:, None] == jnp.arange(EXPERTS, dtype=jnp.int32)[None, :]).astype(jnp.int32)
    slot_rank = lax.optimization_barrier(jnp.sum((jnp.cumsum(one_hot, 0) - one_hot) * one_hot, 1)).astype(jnp.int32)
    capacity = N_EP * N_TP * CAP
    buffer = jnp.zeros((EXPERTS, capacity, D), jnp.bfloat16)
    buffer = buffer.at[flat_routes, slot_rank].set(jnp.repeat(normed, TOP, axis=0))
    outputs = lax.map(expert_rows, (buffer, w_gate, w_up, w_down))
    routed = outputs[flat_routes, slot_rank].reshape(TOKENS, TOP, D)
    mixture = lax.optimization_barrier(jnp.sum(weights[:, :, None] * routed, 1))
    return (residual + mixture).astype(jnp.bfloat16)
```

```python
import functools

import jax
import jax.numpy as jnp
from jax import lax
from jax.experimental import pallas as pl
from jax.experimental.pallas import tpu as pltpu
from jax.sharding import PartitionSpec as P

LANES = 128
LOG2E = 1.4426950408889634
MESH = pl.DeviceIdType.MESH


def attend(queries, new_keys, new_values, key_cache, value_cache, cache_lengths):
    seq_count, kv_count, head_dim, length = key_cache.shape
    new_count = queries.shape[0] // seq_count
    group_size = queries.shape[1] // (kv_count * head_dim)
    row_count = new_count * group_size
    scale = head_dim ** (-0.5)
    query_block = queries.reshape(seq_count, new_count, kv_count, group_size, head_dim)
    query_block = query_block.transpose(0, 2, 1, 3, 4).reshape(
        seq_count, kv_count, row_count, head_dim
    )
    fresh_keys = new_keys.reshape(seq_count, new_count, kv_count, head_dim).transpose(0, 2, 1, 3)
    fresh_values = new_values.reshape(seq_count, new_count, kv_count, head_dim).transpose(
        0, 2, 1, 3
    )
    cache_scores = (
        jnp.einsum("skrd,skdl->skrl", query_block, key_cache, preferred_element_type=jnp.float32)
        * scale
    )
    in_cache = jnp.arange(length)[None, :] < cache_lengths[:, None]
    cache_scores = jnp.where(in_cache[:, None, None, :], cache_scores, -1e30)
    fresh_scores = (
        jnp.einsum("skrd,sknd->skrn", query_block, fresh_keys, preferred_element_type=jnp.float32)
        * scale
    )
    causal = (jnp.arange(row_count) // group_size)[:, None] >= jnp.arange(new_count)[None, :]
    fresh_scores = jnp.where(causal[None, None, :, :], fresh_scores, -1e30)
    row_max = jnp.maximum(
        jnp.max(cache_scores, -1, keepdims=True), jnp.max(fresh_scores, -1, keepdims=True)
    )
    cache_exp = jnp.exp(cache_scores - row_max)
    fresh_exp = jnp.exp(fresh_scores - row_max)
    denom_sum = jnp.sum(cache_exp, -1, keepdims=True) + jnp.sum(fresh_exp, -1, keepdims=True)
    cache_probs = (cache_exp / denom_sum).astype(jnp.bfloat16)
    fresh_probs = (fresh_exp / denom_sum).astype(jnp.bfloat16)
    head_mix = jnp.einsum(
        "skrl,skdl->skrd", cache_probs, value_cache, preferred_element_type=jnp.float32
    )
    head_mix = head_mix + jnp.einsum(
        "skrn,sknd->skrd", fresh_probs, fresh_values, preferred_element_type=jnp.float32
    )
    head_mix = head_mix.reshape(seq_count, kv_count, new_count, group_size, head_dim).transpose(
        0, 2, 1, 3, 4
    )
    return head_mix.reshape(seq_count * new_count, kv_count * group_size * head_dim).astype(
        jnp.bfloat16
    )


def expert_apply(received, w_gate, w_up, w_down):
    width = received.shape[-1]
    flat_rows = received.reshape(-1, width)
    gate_proj = jnp.dot(flat_rows, w_gate[0], preferred_element_type=jnp.float32)
    up_proj = jnp.dot(flat_rows, w_up[0], preferred_element_type=jnp.float32)
    activated = ((up_proj + 1.0) * gate_proj * jax.nn.sigmoid(1.702 * gate_proj)).astype(
        jnp.bfloat16
    )
    partial_out = jnp.dot(activated, w_down[0], preferred_element_type=jnp.float32)
    return partial_out.reshape(received.shape[0], received.shape[1], width)


def layer_kernel(
    ep_size,
    experts,
    lens_hbm,
    query_hbm,
    new_key_hbm,
    new_value_hbm,
    key_hbm,
    value_hbm,
    w_out_hbm,
    hidden_hbm,
    router_hbm,
    routes_hbm,
    gate_hbm,
    up_hbm,
    down_hbm,
    out_ref,
    lens,
    query,
    query_wide,
    fresh_key,
    fresh_value,
    keys,
    values,
    w_out,
    hidden,
    router,
    routes,
    named_all,
    attended,
    part,
    got,
    res,
    rows,
    mixed,
    core_in,
    a_in,
    b_in,
    z_in,
    w_gate,
    w_up,
    w_down,
    load_sem,
    seq_sem,
    first_send,
    first_recv,
    line_send,
    gather_send,
    gather_recv,
    core_send,
    core_recv,
    sum_send,
    a_recv,
    b_recv,
    z_recv,
):
    tp_size, block_rows, width = part.shape
    padded = rows.shape[2]
    base = width // LANES * LANES
    offset = width - base
    line = ep_size // 2
    pair = 2 * line
    unit = 4 * line
    seq_count, head_dim, length = keys.shape
    tokens, query_width = query.shape
    new_count = tokens // seq_count
    seq_block = block_rows // new_count
    cut = (padded // LANES + 1) // 2 * LANES
    bf16 = jnp.bfloat16
    f32 = jnp.float32
    ep = lax.axis_index("ep")
    tp = lax.axis_index("tp")
    x = ep % 2
    z = ep // 2
    core = tp % 2
    y = tp // 2
    x_step = 1 - 2 * x
    y_step = 2 - 4 * y
    mate = tp + 1 - 2 * core
    partner = (ep, mate)
    a_dev = (ep + (1 - core) * x_step, tp + core * y_step)
    b_dev = (ep + core * x_step, tp + (1 - core) * y_step)

    by_distance = [sorted(range(line), key=lambda p: (abs(p - q), p)) for q in range(line)]

    def near(k):
        place = by_distance[0][k] + 0 * z
        for q in range(1, line):
            place = jnp.where(z == q, by_distance[q][k], place)
        return place

    planes = [z] + [near(k) for k in range(1, line)]
    order = [(tp + 2) % tp_size, (mate + 2) % tp_size, mate, tp]

    def block_of(index):
        return pl.ds(pl.multiple_of(index * block_rows, block_rows), block_rows)

    def load(src, dst, index):
        copy = pltpu.make_async_copy(src, dst, load_sem.at[index])
        copy.start()
        return copy

    small = [load(lens_hbm, lens, 0)]
    cache = []
    for i, source in enumerate(order):
        seqs = pl.ds(source * seq_block, seq_block)
        held = pl.ds(i * seq_block, seq_block)
        there = pl.ds(i * block_rows, block_rows)
        moved = []
        for j, (src, dst) in enumerate(
            (
                (query_hbm.at[block_of(source)], query.at[there]),
                (new_key_hbm.at[block_of(source)], fresh_key.at[there]),
                (new_value_hbm.at[block_of(source)], fresh_value.at[there]),
                (key_hbm.at[seqs, 0], keys.at[held]),
                (value_hbm.at[seqs, 0], values.at[held]),
            )
        ):
            copy = pltpu.make_async_copy(src, dst, seq_sem.at[i, j])
            copy.start()
            moved.append(copy)
        cache.append(moved)
    w_out_load = load(w_out_hbm, w_out, 1)
    small.append(load(routes_hbm, routes, 2))
    side = [
        load(hidden_hbm.at[block_of(tp)], hidden, 3),
        load(router_hbm, router.at[pl.ds(0, experts)], 4),
    ]

    peers = [(ep, (tp + k) % tp_size) for k in range(1, tp_size)]
    peers += [(ep + x_step, tp)]
    peers += [(planes[k] * 2 + x, tp) for k in range(1, line)]
    barrier = pltpu.get_barrier_semaphore()
    for peer in peers:
        pl.semaphore_signal(barrier, inc=1, device_id=peer, device_id_type=MESH)

    def send(src, dst, send_sem, recv_sem, device):
        copy = pltpu.make_async_remote_copy(
            src_ref=src,
            dst_ref=dst,
            send_sem=send_sem,
            recv_sem=recv_sem,
            device_id=device,
            device_id_type=MESH,
        )
        copy.start()
        return copy

    for moved in cache:
        for copy in moved:
            copy.wait()
    experts_load = [
        load(gate_hbm.at[0], w_gate.at[pl.ds(0, width)], 5),
        load(up_hbm.at[0], w_up.at[pl.ds(0, width)], 6),
        load(down_hbm.at[0], w_down, 7),
    ]
    for copy in small:
        copy.wait()
    twice = (
        lax.broadcasted_iota(jnp.int32, (head_dim, LANES), 1) % head_dim
        == lax.broadcasted_iota(jnp.int32, (head_dim, LANES), 0)
    ).astype(bf16)
    key_twice = jnp.dot(fresh_key[...], twice, preferred_element_type=f32).astype(bf16)
    value_twice = jnp.dot(fresh_value[...], twice, preferred_element_type=f32).astype(bf16)
    query_wide[...] = query[...].astype(f32)
    group_size = query_width // head_dim
    seq_rows = group_size * new_count
    factor = head_dim**-0.5 * LOG2E
    low_half = lax.broadcasted_iota(jnp.int32, (new_count, LANES), 1) < head_dim
    place = lax.broadcasted_iota(jnp.int32, (seq_rows, length), 1)
    fresh_lane = lax.broadcasted_iota(jnp.int32, (seq_rows, tokens), 1)
    fresh_row = lax.broadcasted_iota(jnp.int32, (seq_rows, tokens), 0) % new_count
    columns = (((1,), (1,)), ((), ()))

    def attend_sequence(s):
        size = lens[order[s // seq_block] * seq_block + s % seq_block]
        mine = slice(s * new_count, (s + 1) * new_count)
        pieces = []
        for low in range(0, query_width, LANES):
            both = query_wide[mine, low : low + LANES]
            pieces += [jnp.where(low_half, both, 0.0), jnp.where(low_half, 0.0, both)]
        left = jnp.concatenate(pieces, axis=0).astype(bf16)
        key = keys[s]
        scores = jnp.dot(left, jnp.concatenate([key, key], axis=0), preferred_element_type=f32)
        scores = jnp.where(place < size, scores * factor, -1e30)
        fresh = lax.dot_general(left, key_twice, columns, preferred_element_type=f32)
        admitted = (fresh_lane >= s * new_count) & (fresh_lane <= s * new_count + fresh_row)
        fresh = jnp.where(admitted, fresh * factor, -1e30)
        top = jnp.maximum(
            jnp.max(scores, -1, keepdims=True), jnp.max(fresh, -1, keepdims=True)
        )
        scores = jnp.exp2(scores - top)
        fresh = jnp.exp2(fresh - top)
        total = jnp.sum(scores, -1, keepdims=True) + jnp.sum(fresh, -1, keepdims=True)
        value = values[s]
        out = lax.dot_general(
            scores.astype(bf16),
            jnp.concatenate([value, value], axis=0),
            columns,
            preferred_element_type=f32,
        )
        out = out + jnp.dot(fresh.astype(bf16), value_twice, preferred_element_type=f32)
        out = out / total
        for i, low in enumerate(range(0, query_width, LANES)):
            first = out[2 * i * new_count : (2 * i + 1) * new_count]
            second = out[(2 * i + 1) * new_count : (2 * i + 2) * new_count]
            attended[mine, low : low + LANES] = jnp.where(low_half, first, second)

    step = 6 * LANES

    def project(first):
        left = attended[first * block_rows : (first + 2) * block_rows].astype(bf16)
        for low in range(0, width, step):
            size = min(step, width - low)
            out = lax.dot_general(
                left, w_out[low : low + size, :], columns, preferred_element_type=f32
            )
            part[first, :, low : low + size] = out[:block_rows].astype(bf16)
            if first == 0:
                part[1, :, low : low + size] = out[block_rows:].astype(bf16)
            else:
                res[:, low : low + size] = out[block_rows:]

    firsts = []

    def first_hop(i):
        firsts.append(
            send(part.at[i], got.at[i], first_send.at[i], first_recv.at[i], (ep, order[i]))
        )

    for s in range(2 * seq_block):
        attend_sequence(s)
    w_out_load.wait()
    project(0)
    pl.semaphore_wait(barrier, len(peers))
    first_hop(0)
    first_hop(1)
    for s in range(2 * seq_block, 4 * seq_block):
        attend_sequence(s)
    project(2)
    first_hop(2)

    for copy in side:
        copy.wait()
    w_gate[width:, :] = jnp.zeros((padded - width, w_gate.shape[1]), bf16)
    w_up[width:, :] = jnp.zeros((padded - width, w_up.shape[1]), bf16)
    res[:, width:] = jnp.zeros((block_rows, padded - width), f32)
    weight_in = router[:experts, :width]
    router_wide = jnp.concatenate(
        [
            jnp.zeros((offset, width), bf16),
            weight_in,
            weight_in,
            jnp.zeros((LANES - offset - 2 * experts, width), bf16),
        ],
        axis=0,
    )
    lane = lax.broadcasted_iota(jnp.int32, (block_rows, LANES), 1)
    second = lane >= offset + experts
    chosen_by = jnp.zeros((experts, tokens), jnp.bool_)
    expert_row = lax.broadcasted_iota(jnp.int32, (experts, tokens), 0)
    for r in range(routes.shape[0]):
        chosen_by = chosen_by | (expert_row == routes[r : r + 1, :])
    lane_row = lax.broadcasted_iota(jnp.int32, (experts, LANES), 1) - offset
    expert_lane = lax.broadcasted_iota(jnp.int32, (experts, LANES), 0)
    spread_to = (lane_row == expert_lane) | (lane_row == expert_lane + experts)
    named_all[...] = lax.dot_general(
        chosen_by.astype(f32),
        spread_to.astype(f32),
        (((0,), (0,)), ((), ())),
        preferred_element_type=f32,
    )
    named = named_all[block_of(tp), :] > 0.5
    own = res[:, :width] + hidden[...].astype(f32)
    for i in (2, 0, 1):
        firsts[i].wait_recv()
        own = own + got[i].astype(f32)
    res[:, :width] = own
    scale = lax.rsqrt(jnp.sum(own * own, -1, keepdims=True) * (1.0 / width) + 1e-05)

    def slot(kind, quarter, plane):
        return (quarter // 2) * unit + kind * pair + (quarter % 2) * line + plane

    def half(h, end):
        return pl.ds(0, cut) if h == 0 else pl.ds(cut, end - cut)

    def row_copy(src, dst, h, send_sem, device):
        return pltpu.make_async_remote_copy(
            src_ref=rows.at[src, :, half(h, padded)],
            dst_ref=rows.at[dst, :, half(h, padded)],
            send_sem=send_sem,
            recv_sem=gather_recv.at[dst, h],
            device_id=device,
            device_id_type=MESH,
        )

    def line_copies(k, h):
        plane = planes[k]
        here = slot(0, 0, plane)
        up = (plane <= z) & (z < line - 1)
        down = (plane >= z) & (z > 0)
        return (
            (up, row_copy(here, here, h, line_send.at[0, k, h], (ep + 2, tp))),
            (down, row_copy(here, here, h, line_send.at[1, k, h], (ep - 2, tp))),
        )

    sent = []

    def hop(src, dst, h, device):
        copy = row_copy(src, dst, h, gather_send.at[dst, h], device)
        copy.start()
        sent.append(copy)

    def forward(quarter, k, h):
        plane = planes[k]
        here = slot(0, quarter, plane)
        if quarter == 0:
            for wanted, copy in line_copies(k, h):
                pl.when(wanted)(copy.start)
            hop(here, slot(0, 1, plane), h, a_dev)
            hop(here, slot(0, 2, plane), h, b_dev)
        if quarter == 1:
            hop(here, slot(0, 3, plane), h, b_dev)
        hop(here, slot(1, quarter, plane), h, partner)

    def arrive(kind, quarter, k, h):
        here = slot(kind, quarter, planes[k])
        row_copy(here, here, h, gather_send.at[here, h], partner).wait_recv()

    mine = slot(0, 0, z)
    rows[mine, :, :cut] = (res[:, :cut] * scale).astype(bf16)
    forward(0, 0, 0)
    normed = (res[...] * scale).astype(bf16)
    logits = lax.dot_general(
        normed[:, :width], router_wide, columns, preferred_element_type=f32
    )
    picked_exp = jnp.where(named, jnp.exp(logits), 0.0)
    denom = jnp.sum(jnp.where(second, 0.0, picked_exp), -1, keepdims=True)
    weights = picked_exp / denom
    high = weights.astype(bf16).astype(f32)
    tail = jnp.where(second, weights - high, high)
    tail = jnp.where(lane < offset, normed[:, base:].astype(f32), tail)
    rows[mine, :, cut:base] = normed[:, cut:base]
    rows[mine, :, base:] = tail.astype(bf16)
    forward(0, 0, 1)

    early = []
    for k in range(line):
        if k + 1 < line:
            early += [(1, k, 0), (0, k + 1, 0), (1, k, 1), (0, k + 1, 1)]
        else:
            early += [(1, k, 0), (1, k, 1)]
        if k == 0:
            early += [(2, 0, 0), (2, 0, 1)]
        if k > 0 and k + 1 < line:
            early += [(2, k, 0), (2, k, 1), (3, k - 1, 0), (3, k - 1, 1)]
    late = [
        (q, k, h)
        for k in range(line)
        for q in (2, 3)
        for h in (0, 1)
        if (q, k, h) not in early
    ]
    for quarter, k, h in early:
        arrive(0, quarter, k, h)
        forward(quarter, k, h)

    share_lane = lax.broadcasted_iota(jnp.int32, (unit * block_rows, LANES), 1)
    chosen = (share_lane == offset + ep) | (share_lane == offset + experts + ep)
    crossing = {}

    def cross(u, h):
        crossing[u, h] = send(
            mixed.at[pl.ds(u * unit + pair, pair), :, half(h, width)],
            core_in.at[pl.ds(u * pair, pair), :, half(h, width)],
            core_send.at[u, h],
            core_recv.at[u, h],
            partner,
        )

    def expert(u):
        start = u * unit
        held = rows[start : start + unit].reshape(unit * block_rows, padded)
        gate = jnp.dot(held, w_gate[...], preferred_element_type=f32)
        up = jnp.dot(held, w_up[...], preferred_element_type=f32)
        active = ((up + 1.0) * gate * jax.nn.sigmoid(1.702 * gate)).astype(bf16)
        share = jnp.sum(jnp.where(chosen, held[:, base:].astype(f32), 0.0), -1, keepdims=True)
        for h, (first, last) in enumerate(((0, cut), (cut, width))):
            for low in range(first, last, step):
                size = min(step, last - low)
                out = lax.dot_general(
                    active, w_down[low : low + size, :], columns, preferred_element_type=f32
                )
                mixed[start : start + unit, :, low : low + size] = (
                    (share * out).astype(bf16).reshape(unit, block_rows, size)
                )
            cross(u, h)

    for copy in experts_load:
        copy.wait()
    for quarter in (0, 1):
        for k in range(line):
            for h in (0, 1):
                arrive(1, quarter, k, h)
    expert(0)
    for quarter, k, h in late:
        arrive(0, quarter, k, h)
        forward(quarter, k, h)

    sums = []

    def total_of(quarter, k, h, parts):
        plane = planes[k]
        there = (quarter // 2) * pair + (quarter % 2) * line + plane
        columns_of = half(h, width)
        total = mixed[slot(0, quarter, plane), :, columns_of].astype(f32)
        total = total + core_in[there, :, columns_of].astype(f32)
        for buffer, index in parts:
            total = total + buffer[index, :, columns_of].astype(f32)
        return total

    def reduce_send(quarter, k, h, parts, dst, recv_sem, device):
        here = slot(0, quarter, planes[k])
        columns_of = half(h, width)
        mixed[here, :, columns_of] = total_of(quarter, k, h, parts).astype(bf16)
        sums.append(
            send(
                mixed.at[here, :, columns_of],
                dst.at[:, columns_of],
                sum_send.at[quarter, k, h],
                recv_sem,
                device,
            )
        )

    def landed(dst, recv_sem):
        pltpu.make_async_remote_copy(
            src_ref=dst,
            dst_ref=dst,
            send_sem=sum_send.at[0, 0, 0],
            recv_sem=recv_sem,
            device_id=partner,
            device_id_type=MESH,
        ).wait_recv()

    far = list(range(line - 1, -1, -1))

    def send_a(quarter, k, h):
        index = (quarter // 2) * line + planes[k]
        reduce_send(quarter, k, h, [], a_in.at[index], a_recv.at[index, h], a_dev)

    def send_b(k, h):
        index = line + planes[k]
        landed(a_in.at[index, :, half(h, width)], a_recv.at[index, h])
        reduce_send(2, k, h, [(a_in, index)], b_in.at[planes[k]], b_recv.at[planes[k], h], b_dev)

    def gathered(k, h):
        plane = planes[k]
        landed(a_in.at[plane, :, half(h, width)], a_recv.at[plane, h])
        landed(b_in.at[plane, :, half(h, width)], b_recv.at[plane, h])
        return [(a_in, plane), (b_in, plane)]

    def send_z(k, h):
        device = (planes[k] * 2 + x, tp)
        reduce_send(0, k, h, gathered(k, h), z_in.at[z], z_recv.at[z, h], device)

    for h in (0, 1):
        crossing[0, h].wait_recv()
    for k in far:
        for h in (0, 1):
            send_a(1, k, h)
    for quarter in (2, 3):
        for k in range(line):
            for h in (0, 1):
                arrive(1, quarter, k, h)
    expert(1)
    for h in (0, 1):
        crossing[1, h].wait_recv()
    for k in far:
        for h in (0, 1):
            send_a(3, k, h)
    second_hop = [(k, h) for k in far for h in (0, 1)]
    last_hop = [(k, h) for k in far[:-1] for h in (0, 1)]
    lead = 5
    for i, (k, h) in enumerate(second_hop):
        send_b(k, h)
        if i + 1 >= lead and last_hop:
            send_z(*last_hop.pop(0))
    for k, h in last_hop:
        send_z(k, h)
    for h in (0, 1):
        columns_of = half(h, width)
        total = res[:, columns_of] + total_of(0, 0, h, gathered(0, h))
        for k in far[:-1]:
            landed(z_in.at[planes[k], :, columns_of], z_recv.at[planes[k], h])
            total = total + z_in[planes[k], :, columns_of].astype(f32)
        out_ref[:, columns_of] = total.astype(bf16)
    for copy in firsts + sent + list(crossing.values()) + sums:
        copy.wait_send()
    for k in range(line):
        for h in (0, 1):
            for wanted, copy in line_copies(k, h):
                pl.when(wanted)(copy.wait_send)


def fused_layer(
    hidden,
    queries,
    new_keys,
    new_values,
    key_cache,
    value_cache,
    cache_lengths,
    w_out,
    w_router,
    routes,
    w_gate,
    w_up,
    w_down,
):
    ep_size = lax.axis_size("ep")
    tp_size = lax.axis_size("tp")
    tokens, width = hidden.shape
    block_rows = tokens // tp_size
    experts = w_router.shape[1]
    hidden_share = w_gate.shape[2]
    base = width // LANES * LANES
    padded = base + LANES
    line = ep_size // 2
    slots = 8 * line
    seq_count, _, head_dim, length = key_cache.shape
    query_width = queries.shape[1]
    any_space = pl.BlockSpec(memory_space=pl.ANY)
    dma = pltpu.SemaphoreType.DMA
    bf16 = jnp.bfloat16
    f32 = jnp.float32
    vmem = pltpu.VMEM
    return pl.pallas_call(
        functools.partial(layer_kernel, ep_size, experts),
        out_shape=jax.ShapeDtypeStruct((block_rows, width), bf16),
        in_specs=[any_space] * 13,
        out_specs=pl.BlockSpec(memory_space=pltpu.VMEM),
        scratch_shapes=[
            pltpu.SMEM((seq_count,), jnp.int32),
            vmem((tokens, query_width), bf16),
            vmem((tokens, query_width), f32),
            vmem((tokens, head_dim), bf16),
            vmem((tokens, head_dim), bf16),
            vmem((seq_count, head_dim, length), bf16),
            vmem((seq_count, head_dim, length), bf16),
            vmem((width, query_width), bf16),
            vmem((block_rows, width), bf16),
            vmem((experts, width), bf16),
            vmem((routes.shape[1], tokens), jnp.int32),
            vmem((tokens, LANES), f32),
            vmem((tokens, query_width), f32),
            vmem((tp_size, block_rows, width), bf16),
            vmem((tp_size - 1, block_rows, width), bf16),
            vmem((block_rows, padded), f32),
            vmem((slots, block_rows, padded), bf16),
            vmem((slots, block_rows, width), bf16),
            vmem((slots // 2, block_rows, width), bf16),
            vmem((2 * line, block_rows, width), bf16),
            vmem((line, block_rows, width), bf16),
            vmem((line, block_rows, width), bf16),
            vmem((padded, hidden_share), bf16),
            vmem((padded, hidden_share), bf16),
            vmem((width, hidden_share), bf16),
            dma((8,)),
            dma((tp_size, 5)),
            dma((tp_size - 1,)),
            dma((tp_size - 1,)),
            dma((2, line, 2)),
            dma((slots, 2)),
            dma((slots, 2)),
            dma((2, 2)),
            dma((2, 2)),
            dma((4, line, 2)),
            dma((2 * line, 2)),
            dma((line, 2)),
            dma((line, 2)),
        ],
        compiler_params=pltpu.CompilerParams(
            collective_id=0, has_side_effects=True, vmem_limit_bytes=67043328
        ),
    )(
        cache_lengths,
        queries,
        new_keys,
        new_values,
        key_cache,
        value_cache,
        w_out.T,
        hidden,
        w_router.T,
        routes.T,
        w_gate,
        w_up,
        jnp.swapaxes(w_down, 1, 2),
    )


def body(
    hidden,
    queries,
    new_keys,
    new_values,
    key_cache,
    value_cache,
    cache_lengths,
    w_out,
    w_router,
    routes,
    w_gate,
    w_up,
    w_down,
):
    tp_size = lax.axis_size("tp")
    tp_index = lax.axis_index("tp")
    width = hidden.shape[1]
    block_rows = hidden.shape[0] // tp_size
    top_count = routes.shape[1]
    experts = w_router.shape[1]
    capacity = min(block_rows, max(2, (2 * block_rows * top_count + experts - 1) // experts))
    start_row = tp_index * block_rows
    fits = width % LANES + 2 * experts <= LANES and experts == lax.axis_size("ep")
    seq_count, kv_count, head_dim, _ = key_cache.shape
    new_count = hidden.shape[0] // seq_count
    fits = fits and kv_count == 1 and 2 * head_dim == LANES and new_count == 8
    fits = fits and block_rows == 2 * new_count
    if capacity >= block_rows and tp_size == 4 and experts % 2 == 0 and experts > 2 and fits:
        return fused_layer(
            hidden,
            queries,
            new_keys,
            new_values,
            key_cache,
            value_cache,
            cache_lengths,
            w_out,
            w_router,
            routes,
            w_gate,
            w_up,
            w_down,
        )
    attended = attend(queries, new_keys, new_values, key_cache, value_cache, cache_lengths)
    partial_value = jnp.dot(attended, w_out, preferred_element_type=jnp.float32)
    summed = lax.psum_scatter(
        partial_value.astype(jnp.bfloat16), "tp", scatter_dimension=0, tiled=True
    ).astype(jnp.float32)
    residual = (
        lax.dynamic_slice_in_dim(hidden, start_row, block_rows, 0).astype(jnp.float32) + summed
    )
    local_routes = lax.dynamic_slice_in_dim(routes, start_row, block_rows, 0)
    block_count = 1
    normed = (
        residual * lax.rsqrt(jnp.mean(residual * residual, -1, keepdims=True) + 1e-05)
    ).astype(jnp.bfloat16)
    logits = jnp.dot(normed, w_router, preferred_element_type=jnp.float32)
    expert_ids = jnp.arange(experts, dtype=jnp.int32)
    matches = local_routes[:, :, None] == expert_ids[None, None, :]
    picked = jnp.sum(jnp.where(matches, logits[:, None, :], 0.0), -1)
    picked_exp = jnp.exp(picked)
    weights = picked_exp / jnp.sum(picked_exp, -1, keepdims=True)
    flat_routes = local_routes.reshape(-1)
    one_hot = (
        flat_routes.reshape(block_count, block_rows * top_count)[:, :, None]
        == expert_ids[None, None, :]
    ).astype(jnp.int32)
    slot_rank = jnp.sum((jnp.cumsum(one_hot, 1) - one_hot) * one_hot, -1)
    slot_index = (
        slot_rank + (jnp.arange(block_count, dtype=jnp.int32) * capacity)[:, None]
    ).reshape(-1)
    outgoing = jnp.zeros((experts, block_count * capacity, width), jnp.bfloat16)
    outgoing = outgoing.at[flat_routes, slot_index].set(jnp.repeat(normed, top_count, axis=0))
    grouped = expert_apply(
        lax.all_gather(
            lax.all_to_all(outgoing, "ep", split_axis=0, concat_axis=0, tiled=True),
            "tp",
            axis=1,
            tiled=True,
        ),
        w_gate,
        w_up,
        w_down,
    )
    group_total = lax.psum_scatter(
        grouped.astype(jnp.bfloat16), "tp", scatter_dimension=1, tiled=True
    ).astype(jnp.float32)
    returned = lax.all_to_all(
        group_total.astype(jnp.bfloat16), "ep", split_axis=0, concat_axis=0, tiled=True
    ).astype(group_total.dtype)
    routed = returned[flat_routes, slot_index].reshape(-1, top_count, width)
    mixture = jnp.sum(weights[:, :, None] * routed, 1)
    return (residual + mixture).astype(jnp.bfloat16)


def solution(mesh):
    return jax.shard_map(
        body,
        mesh=mesh,
        in_specs=(
            P("ep", None),
            P("ep", "tp"),
            P("ep", "tp"),
            P("ep", "tp"),
            P("ep", "tp", None, None),
            P("ep", "tp", None, None),
            P("ep"),
            P("tp", None),
            P(),
            P("ep", None),
            P("ep", None, "tp"),
            P("ep", None, "tp"),
            P("ep", "tp", None),
        ),
        out_specs=P(("ep", "tp"), None),
        check_vma=False,
    )
```
